32 devices in a mesh: blk: 16 (over z, y, core), dp: 2 (over x).
Axes of the slice: x: 2, y: 2, z: 4, core: 2. Of those that a mesh axis runs over, the one named last changes fastest.
Arguments:
- query_feats: bfloat16 [2, 6144, 1024], P('dp', 'blk'), may hold values from -12 to 12
- item_feats: bfloat16 [2, 6144, 1024], P('dp', 'blk'), may hold values from -12 to 12
- item_ids: int32 [2, 6144], P('dp', 'blk'), may hold values from 0 to 1048575
- bucket_ids: int32 [2, 6144], P('dp', 'blk'), may hold values from 0 to 255
- bucket_logq: float32 [256], replicated, may hold values from -7 to -5.5
- query_tower: bfloat16 [1024, 256], replicated, may hold values from -0.1875 to 0.1875
- item_tower: bfloat16 [1024, 256], replicated, may hold values from -0.1875 to 0.1875
Outputs:
- grad_query_tower: float32 [1024, 256], replicated
- grad_item_tower: float32 [1024, 256], replicated
- loss: float32 [], replicated
The draws below stay inside these ranges and needn't reach their ends.
All inputs are finite; a program needn't handle non-finite values.
Results may differ from the reference program's by a relative error of at most 0.0041.
Values may be sent and summed in bfloat16 or wider, within the bound.
A program may use at most 128 MiB of HBM per device.

```python
import math
import jax
import jax.numpy as jnp
import numpy as np
from jax import lax

F = 1024
E = 256
TOK_DEV = 384
NB = 256
ID_RANGE = 1048576
GROUP = 6144
N_DP = 2


def paired_feats(key):
    base = jax.random.fold_in(key, 101)
    keys = [jax.random.fold_in(base, number) for number in range(8)]
    shape = (N_DP, GROUP, F)
    query_side = jax.random.truncated_normal(keys[0], -6.0, 6.0, shape, jnp.float32)
    item_side = jax.random.truncated_normal(keys[1], -6.0, 6.0, shape, jnp.float32)
    return (query_side, item_side)


def paired_towers(key):
    base = jax.random.fold_in(key, 202)
    first = jax.random.fold_in(base, 1)
    second = jax.random.fold_in(base, 2)
    factor = 1.0 / math.sqrt(F)
    query_weight = jax.random.truncated_normal(first, -6.0, 6.0, (F, E), jnp.float32) * factor
    item_weight = jax.random.truncated_normal(second, -6.0, 6.0, (F, E), jnp.float32) * factor
    return (query_weight, item_weight)


def draw_query_feats(key, part):
    return paired_feats(key)[0].astype(jnp.bfloat16)


def draw_item_feats(key, part):
    return paired_feats(key)[1].astype(jnp.bfloat16)


def draw_query_tower(key, part):
    return paired_towers(key)[0].astype(jnp.bfloat16)


def draw_item_tower(key, part):
    return paired_towers(key)[1].astype(jnp.bfloat16)


def plant(values, key, least, high):
    spot = [jax.random.randint(jax.random.fold_in(key, axis), (), 0, length) for axis, length in enumerate(values.shape)]
    main_axis = values.shape.index(max(values.shape))
    neighbour = spot[:main_axis] + [(spot[main_axis] + 1) % values.shape[main_axis]] + spot[main_axis + 1:]
    return values.at[tuple(spot)].set(least).at[tuple(neighbour)].set(high)


def ranked_wide(stream_key, extent, number_of, slope):
    portions = [min(1 << octave, number_of + 1 - (1 << octave)) * (1 << 20) // math.isqrt((1 << octave) ** slope) + 1 for octave in range((number_of + 1).bit_length()) if 1 << octave <= number_of]
    deviation = 1 + sum(portions) // (1 << 30)
    listing = np.cumsum(np.array([max(1, weight // deviation) for weight in portions]))
    lot = jax.random.randint(jax.random.fold_in(stream_key, 1), extent, 0, int(listing[len(portions) - 1]))
    start = jnp.left_shift(1, jnp.searchsorted(jnp.asarray(listing, jnp.int32), lot, side="right").astype(jnp.int32))
    standing = start - 1 + jax.random.randint(jax.random.fold_in(stream_key, 4), extent, 0, 1 << 30) % jnp.minimum(start, number_of + 1 - start)
    return jax.random.permutation(jax.random.fold_in(stream_key, 2), number_of)[standing].astype(jnp.int32)


def setup_inputs(seed: int = 0) -> dict:
    key_list = jax.random.split(jax.random.key(seed), 8)
    query_feats = draw_query_feats(jax.random.fold_in(key_list[7], 71), 0)
    item_feats = draw_item_feats(jax.random.fold_in(key_list[7], 71), 0)
    item_ids = plant(ranked_wide(key_list[2], (N_DP, GROUP), ID_RANGE, 2), jax.random.fold_in(key_list[2], 3), 0, ID_RANGE - 1).astype(jnp.int32)
    bucket_ids = plant(jax.random.randint(key_list[3], (N_DP, GROUP), 0, NB), jax.random.fold_in(key_list[3], 1), 0, NB - 1).astype(jnp.int32)
    bucket_logq = jnp.clip(jax.random.uniform(key_list[4], (NB,), jnp.float32, -7.0, -5.5), -7.0, -5.5)
    query_tower = draw_query_tower(jax.random.fold_in(key_list[7], 71), 0)
    item_tower = draw_item_tower(jax.random.fold_in(key_list[7], 71), 0)
    return dict(query_feats=query_feats, item_feats=item_feats, item_ids=item_ids, bucket_ids=bucket_ids, bucket_logq=bucket_logq, query_tower=query_tower, item_tower=item_tower)


EXCLUDED = -1e+30

def contract_last(left, right):
    return lax.dot_general(left, right, (((1,), (1,)), ((), ())), preferred_element_type=jnp.float32)

def contract_first(left, right):
    return lax.dot_general(left, right, (((0,), (0,)), ((), ())), preferred_element_type=jnp.float32)

def group_terms(query_input, item_input, group_ids, group_buckets, bucket_logq, query_tower, item_tower):
    scaling = 1.0 / math.sqrt(E)
    query_vecs = jnp.dot(query_input, query_tower, preferred_element_type=jnp.float32).astype(jnp.bfloat16)
    item_vecs = jnp.dot(item_input, item_tower, preferred_element_type=jnp.float32).astype(jnp.bfloat16)
    correction = bucket_logq[group_buckets]
    columns = jnp.arange(GROUP, dtype=jnp.int32)
    blocks = GROUP // TOK_DEV
    query_blocks = query_vecs.reshape(blocks, TOK_DEV, E)
    id_blocks = group_ids.reshape(blocks, TOK_DEV)
    item_blocks = item_vecs.reshape(blocks, TOK_DEV, E)

    def block_step(item_sums, inputs):
        index, block_vecs, block_ids, block_items = inputs
        offset = (index * TOK_DEV).astype(jnp.int32)
        scores = contract_last(block_vecs, item_vecs) * scaling - correction[None, :]
        rows_global = offset + jnp.arange(TOK_DEV, dtype=jnp.int32)
        duplicate = (group_ids[None, :] == block_ids[:, None]) & (columns[None, :] != rows_global[:, None])
        masked = jnp.where(duplicate, EXCLUDED, scores)
        peaks = lax.optimization_barrier(jnp.max(masked, axis=1))
        log_total = peaks + jnp.log(lax.optimization_barrier(jnp.sum(jnp.exp(masked - peaks[:, None]), axis=1)))
        softmax = jnp.exp(masked - log_total[:, None]).astype(jnp.bfloat16)
        positive = jnp.diagonal(lax.dynamic_slice_in_dim(scores, offset, TOK_DEV, 1))
        loss_local = jnp.sum(log_total - positive)
        query_grad = ((jnp.dot(softmax, item_vecs, preferred_element_type=jnp.float32) - block_items.astype(jnp.float32)) * scaling).astype(jnp.bfloat16)
        item_sums = item_sums + contract_first(softmax, block_vecs)
        return (item_sums, (query_grad, loss_local))
    initial = jnp.zeros((GROUP, E), jnp.float32)
    item_sums, (query_grads, losses) = lax.scan(block_step, initial, (jnp.arange(blocks, dtype=jnp.int32), query_blocks, id_blocks, item_blocks))
    query_grads = query_grads.reshape(GROUP, E)
    item_grad = ((item_sums - query_vecs.astype(jnp.float32)) * scaling).astype(jnp.bfloat16)
    tower_query = contract_first(query_input, query_grads)
    tower_item = contract_first(item_input, item_grad)
    return (tower_query, tower_item, jnp.sum(losses))

def reference(query_feats, item_feats, item_ids, bucket_ids, bucket_logq, query_tower, item_tower):

    def one_group(inputs):
        return group_terms(inputs[0], inputs[1], inputs[2], inputs[3], bucket_logq, query_tower, item_tower)
    tower_query, tower_item, losses = lax.map(one_group, (query_feats, item_feats, item_ids, bucket_ids))
    return (lax.optimization_barrier(jnp.sum(tower_query, axis=0)), lax.optimization_barrier(jnp.sum(tower_item, axis=0)), jnp.sum(losses) / (N_DP * GROUP))
```

```python
import functools
import math

import jax
import jax.numpy as jnp
from jax import lax
from jax.experimental import pallas as pl
from jax.experimental.pallas import tpu as pltpu
from jax.sharding import PartitionSpec as P

EXCLUDED = -1e30
LANES = 128
LOW = 4
F32 = jnp.float32
BF16 = jnp.bfloat16


def contract_last(left, right):
    return lax.dot_general(left, right, (((1,), (1,)), ((), ())), preferred_element_type=F32)


def matmul(left, right):
    return jnp.dot(left, right, preferred_element_type=F32)


def as_column(row):
    return jnp.transpose(jnp.broadcast_to(row, (LANES, row.shape[1])))


def as_wide_column(row, width):
    column = as_column(row)
    return jnp.concatenate([column] * (width // LANES), axis=1)


def kernel(
    high, parts,
    qx_ref, ix_ref, ids_ref, buckets_ref, logq_ref, qw_ref, iw_ref,
    grad_q_ref, grad_i_ref, loss_ref,
    q_all, i_all, meta_q, meta_i, i_turned, qx_turned, ix_turned,
    id_col, corr_col, score, weight, q_scaled,
    stats, o_send, o_recv, o_own, u_send, u_recv, u_own,
    grads, half_recv, acc, send1, recv1, acc1, send2, recv2, acc2, send3, recv3, full, loss_buf,
    sem_qs, sem_qr, sem_is, sem_ir, sem_ms, sem_mr, sem_ns, sem_nr,
    sem_ss, sem_sr, sem_os, sem_or, sem_us, sem_ur,
    sem_hs, sem_hr, sem_1s, sem_1r, sem_2s, sem_2r, sem_3s, sem_3r,
    sem_ls, sem_lr, sem_g3s, sem_g3r, sem_g2s, sem_g2r, sem_g1s, sem_g1r, sem_g0s, sem_g0r,
):
    rows, width = qx_ref.shape
    embed = qw_ref.shape[1]
    group_items = LOW * rows
    scaling = 1.0 / math.sqrt(embed)
    me = lax.axis_index("blk")
    part = lax.axis_index("dp")
    hi, lo = me // LOW, me % LOW
    mid, core = lo // 2, lo % 2

    def by_high(k):
        return {"blk": lax.rem(hi + k, high) * LOW + lo}

    def by_low(k):
        return {"blk": hi * LOW + lax.rem(lo + k, LOW)}

    def by_part(k):
        return {"dp": lax.rem(part + k, parts)}

    by_core = {"blk": hi * LOW + mid * 2 + (1 - core)}
    by_mid = {"blk": hi * LOW + (1 - mid) * 2 + core}

    def send(src, dst, send_sem, recv_sem, device):
        copy = pltpu.make_async_remote_copy(
            src_ref=src, dst_ref=dst, send_sem=send_sem, recv_sem=recv_sem,
            device_id=device, device_id_type=pl.DeviceIdType.MESH,
        )
        copy.start()
        return copy

    barrier = pltpu.get_barrier_semaphore()
    greeted = [by_high(k) for k in range(1, high)] + [by_low(k) for k in range(1, LOW)]
    greeted += [by_part(k) for k in range(1, parts)]
    for device in greeted:
        pl.semaphore_signal(barrier, inc=1, device_id=device, device_id_type=pl.DeviceIdType.MESH)

    q_all[0] = matmul(qx_ref[...], qw_ref[...]).astype(BF16)
    logq_col = as_column(logq_ref[...])
    count = logq_col.shape[0]
    pieces = []
    for c in range(rows // LANES):
        lane = slice(c * LANES, (c + 1) * LANES)
        bucket = lax.broadcasted_iota(jnp.int32, (count, LANES), 0)
        chosen = jnp.where(bucket == buckets_ref[:, lane], logq_col, 0.0)
        pieces.append(jnp.sum(chosen, axis=0, keepdims=True))
    meta_q[0, 0:1, :] = ids_ref[...].astype(F32)
    meta_q[0, 1:2, :] = jnp.concatenate(pieces, axis=1)
    meta_q[0, 2:8, :] = jnp.zeros((6, rows), F32)
    meta_i[0] = meta_q[0]
    pl.semaphore_wait(barrier, len(greeted))

    copies_q, copies_m, copies_i, copies_n = [], [], [], []
    for k in range(1, high):
        copies_q.append(send(q_all.at[0], q_all.at[k], sem_qs.at[k], sem_qr.at[k], by_high(k)))
        copies_m.append(send(meta_q.at[0], meta_q.at[k], sem_ms.at[k], sem_mr.at[k], by_high(k)))
    i_all[0] = matmul(ix_ref[...], iw_ref[...]).astype(BF16)
    for k in range(1, LOW):
        copies_n.append(send(meta_i.at[0], meta_i.at[k], sem_ns.at[k], sem_nr.at[k], by_low(k)))
        copies_i.append(send(i_all.at[0], i_all.at[k], sem_is.at[k], sem_ir.at[k], by_low(k)))

    qx_turned[...] = jnp.transpose(qx_ref[...])
    ix_turned[...] = jnp.transpose(ix_ref[...])

    for k in range(LOW):
        if k:
            copies_i[k - 1].wait_recv()
            copies_n[k - 1].wait_recv()
        span = slice(k * rows, (k + 1) * rows)
        i_turned[:, span] = jnp.transpose(i_all[k])
        id_col[span, :] = as_column(meta_i[k, 0:1, :])
        corr_col[span, :] = as_column(meta_i[k, 1:2, :])

    step_rows = 32
    lane_chunks = rows // LANES
    copies_o = []
    positive = None
    for k in range(high):
        if k:
            copies_q[k - 1].wait_recv()
            copies_m[k - 1].wait_recv()
        for j in range(LOW):
            score[j * rows:(j + 1) * rows, :] = contract_last(i_all[j], q_all[k])
        id_row = meta_q[k, 0:1, :]

        def mask_step(own, step, peak):
            start = pl.multiple_of(step * step_rows, step_rows)
            span = pl.ds(start, step_rows)
            new, diag = [], []
            for c in range(lane_chunks):
                lane = slice(c * LANES, (c + 1) * LANES)
                value = score[span, lane] * scaling - corr_col[span, :]
                same = id_col[span, :] == id_row[:, lane]
                if own:
                    row = lax.broadcasted_iota(jnp.int32, (step_rows, LANES), 0) + start
                    col = lax.broadcasted_iota(jnp.int32, (step_rows, LANES), 1) + c * LANES
                    on_diag = row == col
                    diag.append(jnp.sum(jnp.where(on_diag, value, 0.0).reshape(step_rows // 8, 8, LANES), axis=0))
                    same = same & jnp.logical_not(on_diag)
                value = jnp.where(same, EXCLUDED, value)
                score[span, lane] = value
                new.append(jnp.max(value.reshape(step_rows // 8, 8, LANES), axis=0))
            top = jnp.concatenate(new, axis=1)
            if own:
                return jnp.maximum(peak[0], top), peak[1] + jnp.concatenate(diag, axis=1)
            return jnp.maximum(peak, top)

        peak = jnp.full((8, rows), EXCLUDED, F32)
        total_steps = group_items // step_rows
        first = 0
        if k == 0:
            first = rows // step_rows
            peak, diag = lax.fori_loop(
                0, first, functools.partial(mask_step, True), (peak, jnp.zeros((8, rows), F32))
            )
            positive = jnp.sum(diag, axis=0, keepdims=True)
        peak = lax.fori_loop(first, total_steps, functools.partial(mask_step, False), peak)
        peak = jnp.max(peak, axis=0, keepdims=True)

        def exp_step(step, total):
            span = pl.ds(pl.multiple_of(step * step_rows, step_rows), step_rows)
            value = jnp.exp(score[span, :] - peak)
            weight[span, k * rows:(k + 1) * rows] = value.astype(BF16)
            return total + jnp.sum(value.reshape(step_rows // 8, 8, rows), axis=0)

        total = lax.fori_loop(0, total_steps, exp_step, jnp.zeros((8, rows), F32))
        stats[0, 2 * k:2 * k + 1, :] = peak
        stats[0, 2 * k + 1:2 * k + 2, :] = jnp.sum(total, axis=0, keepdims=True)
        partial = matmul(i_turned[...], weight[:, k * rows:(k + 1) * rows])
        if k == 0:
            o_own[...] = partial
        else:
            o_send[k] = partial.astype(BF16)
            copies_o.append(
                send(o_send.at[k], o_recv.at[k], sem_os.at[k], sem_or.at[k], by_high(high - k))
            )

    copies_s = [
        send(stats.at[0], stats.at[k], sem_ss.at[k], sem_sr.at[k], by_high(k)) for k in range(1, high)
    ]
    for copy in copies_s:
        copy.wait_recv()
    log_total = []
    for k in range(high):
        peaks = [stats[d, 2 * ((k - d) % high):2 * ((k - d) % high) + 1, :] for d in range(high)]
        sums = [stats[d, 2 * ((k - d) % high) + 1:2 * ((k - d) % high) + 2, :] for d in range(high)]
        top = functools.reduce(jnp.maximum, peaks)
        whole = functools.reduce(jnp.add, [s * jnp.exp(p - top) for p, s in zip(peaks, sums)])
        log_total.append(top + jnp.log(whole))
        factor = jnp.exp(peaks[0] - log_total[k])
        q_scaled[k * rows:(k + 1) * rows, :] = (
            q_all[k].astype(F32) * as_wide_column(factor, embed)
        ).astype(BF16)

    copies_u = []
    for j in list(range(1, LOW)) + [0]:
        sums = matmul(weight[j * rows:(j + 1) * rows, :], q_scaled[...])
        if j:
            u_send[j] = sums.astype(BF16)
            copies_u.append(
                send(u_send.at[j], u_recv.at[j], sem_us.at[j], sem_ur.at[j], by_low(LOW - j))
            )
        else:
            u_own[...] = sums

    own_total = o_own[...] * jnp.exp(stats[0, 0:1, :] - log_total[0])
    for k in range(1, high):
        copies_o[k - 1].wait_recv()
        d = high - k
        own_total += o_recv[k].astype(F32) * jnp.exp(stats[d, 2 * k:2 * k + 1, :] - log_total[0])
    query_grad = ((jnp.transpose(own_total) - i_all[0].astype(F32)) * scaling).astype(BF16)
    grads[0] = matmul(qx_turned[...], query_grad)
    lost = jnp.sum(log_total[0] - positive, axis=1, keepdims=True)

    sums = u_own[...]
    for j in range(1, LOW):
        copies_u[j - 1].wait_recv()
        sums += u_recv[j].astype(F32)
    item_grad = ((sums - q_all[0].astype(F32)) * scaling).astype(BF16)
    grads[1] = matmul(ix_turned[...], item_grad)

    pending = copies_q + copies_m + copies_i + copies_n + copies_o + copies_s + copies_u

    loss_buf[0] = jnp.broadcast_to(lost, (8, LANES))
    slot = 0

    def loss_round(partners):
        nonlocal slot
        base, copies = slot, []
        for n, device in enumerate(partners):
            at = base + 1 + n
            copies.append(send(loss_buf.at[base], loss_buf.at[at], sem_ls.at[at], sem_lr.at[at], device))
        return base, copies

    def loss_sum(base, copies):
        nonlocal slot
        value = loss_buf[base]
        for n, copy in enumerate(copies):
            copy.wait_recv()
            value += loss_buf[base + 1 + n]
        pending.extend(copies)
        slot = base + 1 + len(copies)
        loss_buf[slot] = value

    copy = send(grads.at[1 - core], half_recv, sem_hs.at[0], sem_hr.at[0], by_core)
    base, copies = loss_round([by_core])
    copy.wait_recv()
    acc[...] = grads[core].reshape(acc.shape) + half_recv[...].reshape(acc.shape)
    pending.append(copy)
    loss_sum(base, copies)

    moved = []
    for k in range(1, parts):
        send1[k] = acc[lax.rem(part + k, parts)].astype(BF16)
        moved.append(send(send1.at[k], recv1.at[k], sem_1s.at[k], sem_1r.at[k], by_part(k)))
    base, copies = loss_round([by_part(k) for k in range(1, parts)])
    value = acc[part]
    for k in range(1, parts):
        moved[k - 1].wait_recv()
        value += recv1[k].astype(F32)
    acc1[...] = value.reshape(acc1.shape)
    pending.extend(moved)
    loss_sum(base, copies)

    send2[...] = acc1[1 - mid].astype(BF16)
    copy = send(send2, recv2, sem_2s.at[0], sem_2r.at[0], by_mid)
    base, copies = loss_round([by_mid])
    copy.wait_recv()
    acc2[...] = (acc1[mid] + recv2[...].astype(F32)).reshape(acc2.shape)
    pending.append(copy)
    loss_sum(base, copies)

    moved = []
    for k in range(1, high):
        send3[k] = acc2[lax.rem(hi + k, high)].astype(BF16)
        moved.append(send(send3.at[k], recv3.at[k], sem_3s.at[k], sem_3r.at[k], by_high(k)))
    base, copies = loss_round([by_high(k) for k in range(1, high)])
    value = acc2[hi]
    for k in range(1, high):
        moved[k - 1].wait_recv()
        value += recv3[k].astype(F32)
    full[core, part, mid, hi] = value.astype(BF16)
    pending.extend(moved)
    loss_sum(base, copies)

    place = full.at[core, part, mid, hi]
    moved = [send(place, place, sem_g3s.at[k], sem_g3r.at[k], by_high(k)) for k in range(1, high)]
    for copy in moved:
        copy.wait_recv()
    pending.extend(moved)
    place = full.at[core, part, mid]
    copy = send(place, place, sem_g2s.at[0], sem_g2r.at[0], by_mid)
    copy.wait_recv()
    pending.append(copy)
    place = full.at[core, part]
    moved = [send(place, place, sem_g1s.at[k], sem_g1r.at[k], by_part(k)) for k in range(1, parts)]
    for copy in moved:
        copy.wait_recv()
    pending.extend(moved)
    place = full.at[core]
    copy = send(place, place, sem_g0s.at[0], sem_g0r.at[0], by_core)
    copy.wait_recv()
    pending.append(copy)

    piece = full.shape[4]
    at = 0
    for a in range(parts):
        for b in range(2):
            for c in range(high):
                grad_q_ref[at:at + piece, :] = full[0, a, b, c].astype(F32)
                grad_i_ref[at:at + piece, :] = full[1, a, b, c].astype(F32)
                at += piece
    loss_ref[...] = loss_buf[slot] * (1.0 / (parts * high * LOW * rows))
    for copy in pending:
        copy.wait_send()


def on_device(high, parts, query_feats, item_feats, item_ids, bucket_ids, bucket_logq, query_tower, item_tower):
    rows, width = query_feats.shape[1:]
    embed = query_tower.shape[1]
    items = LOW * rows
    stat_rows = -(-2 * high // 8) * 8
    rounds = 1 + 1 + 1 + (parts - 1) + 1 + 1 + 1 + (high - 1) + 1
    r1 = width // parts
    r2 = r1 // 2
    r3 = r2 // high
    vmem, dma = pltpu.VMEM, pltpu.SemaphoreType.DMA
    block = (rows, embed)
    scratch = [
        vmem((high,) + block, BF16), vmem((LOW,) + block, BF16),
        vmem((high, 8, rows), F32), vmem((LOW, 8, rows), F32),
        vmem((embed, items), BF16), vmem((width, rows), BF16), vmem((width, rows), BF16),
        vmem((items, LANES), F32), vmem((items, LANES), F32),
        vmem((items, rows), F32), vmem((items, high * rows), BF16), vmem((high * rows, embed), BF16),
        vmem((high, stat_rows, rows), F32),
        vmem((high, embed, rows), BF16), vmem((high, embed, rows), BF16), vmem((embed, rows), F32),
        vmem((LOW,) + block, BF16), vmem((LOW,) + block, BF16), vmem(block, F32),
        vmem((2, width, embed), F32), vmem((width, embed), F32), vmem((parts, r1, embed), F32),
        vmem((parts, r1, embed), BF16), vmem((parts, r1, embed), BF16), vmem((2, r2, embed), F32),
        vmem((r2, embed), BF16), vmem((r2, embed), BF16), vmem((high, r3, embed), F32),
        vmem((high, r3, embed), BF16), vmem((high, r3, embed), BF16),
        vmem((2, parts, 2, high, r3, embed), BF16), vmem((rounds, 8, LANES), F32),
    ]
    scratch += [dma((n,)) for n in (high, high, LOW, LOW, high, high, LOW, LOW)]
    scratch += [dma((n,)) for n in (high, high, high, high, LOW, LOW)]
    scratch += [dma((n,)) for n in (1, 1, parts, parts, 1, 1, high, high)]
    scratch += [dma((n,)) for n in (rounds, rounds, high, high, 1, 1, parts, parts, 1, 1)]
    grad_q, grad_i, loss = pl.pallas_call(
        functools.partial(kernel, high, parts),
        out_shape=(
            jax.ShapeDtypeStruct((width, embed), F32),
            jax.ShapeDtypeStruct((width, embed), F32),
            jax.ShapeDtypeStruct((8, LANES), F32),
        ),
        in_specs=[pl.BlockSpec(memory_space=pltpu.VMEM)] * 7,
        out_specs=[pl.BlockSpec(memory_space=pltpu.VMEM)] * 3,
        scratch_shapes=scratch,
        compiler_params=pltpu.CompilerParams(
            collective_id=0, has_side_effects=True, vmem_limit_bytes=60 * 1024 * 1024
        ),
        name="two_tower",
    )(
        query_feats[0], item_feats[0], item_ids, bucket_ids, bucket_logq[None, :], query_tower, item_tower
    )
    return grad_q, grad_i, loss[0, 0]


def solution(mesh):
    high = mesh.shape["blk"] // LOW
    return jax.shard_map(
        functools.partial(on_device, high, mesh.shape["dp"]),
        mesh=mesh,
        in_specs=(
            P("dp", "blk", None), P("dp", "blk", None), P("dp", "blk"), P("dp", "blk"), P(), P(), P(),
        ),
        out_specs=(P(), P(), P()),
        check_vma=False,
    )
```

```python
import functools
import math

import jax
import jax.numpy as jnp
from jax import lax
from jax.experimental import pallas as pl
from jax.experimental.pallas import tpu as pltpu
from jax.sharding import PartitionSpec as P

EXCLUDED = -1e30
LANES = 128
LOW = 4
F32 = jnp.float32
BF16 = jnp.bfloat16


def contract_last(left, right):
    return lax.dot_general(left, right, (((1,), (1,)), ((), ())), preferred_element_type=F32)


def matmul(left, right):
    return jnp.dot(left, right, preferred_element_type=F32)


def as_column(row):
    return jnp.transpose(jnp.broadcast_to(row, (LANES, row.shape[1])))


def as_wide_column(row, width):
    column = as_column(row)
    return jnp.concatenate([column] * (width // LANES), axis=1)


def kernel(
    high, parts,
    qx_hbm, ix_hbm, ids_ref, buckets_ref, logq_ref, qw_hbm, iw_hbm,
    grad_ref, loss_ref,
    qx_ref, ix_ref, qw_ref, iw_ref,
    q_all, i_all, meta_q, meta_i, i_turned, qx_turned, ix_turned,
    id_col, corr_col, score, weight, q_scaled,
    stats, o_send, o_recv, o_own, u_send, u_recv, u_own, u_far,
    grads, half_recv, acc, send1, recv1, acc1, send2, recv2, acc2, send3, recv3,
    sendb, recvb, accb, sendc, recvc, full, loss_buf,
    sem_in, sem_out,
    sem_qs, sem_qr, sem_is, sem_ir, sem_ms, sem_mr, sem_ns, sem_nr,
    sem_ss, sem_sr, sem_os, sem_or, sem_us, sem_ur,
    sem_hs, sem_hr, sem_1s, sem_1r, sem_2s, sem_2r, sem_3s, sem_3r,
    sem_bs, sem_br, sem_cs, sem_cr,
    sem_ls, sem_lr, sem_g3s, sem_g3r, sem_g2s, sem_g2r, sem_g1s, sem_g1r, sem_g0s, sem_g0r,
):
    rows, width = qx_ref.shape
    embed = qw_ref.shape[1]
    scaling = 1.0 / math.sqrt(embed)
    me = lax.axis_index("blk")
    part = lax.axis_index("dp")
    hi, lo = me // LOW, me % LOW
    mid, core = lo // 2, lo % 2

    def by_high(k):
        return {"blk": lax.rem(hi + k, high) * LOW + lo}

    def by_part(k):
        return {"dp": lax.rem(part + k, parts)}

    by_core = {"blk": hi * LOW + mid * 2 + (1 - core)}
    by_mid = {"blk": hi * LOW + (1 - mid) * 2 + core}

    def send(src, dst, send_sem, recv_sem, device):
        copy = pltpu.make_async_remote_copy(
            src_ref=src, dst_ref=dst, send_sem=send_sem, recv_sem=recv_sem,
            device_id=device, device_id_type=pl.DeviceIdType.MESH,
        )
        copy.start()
        return copy

    barrier = pltpu.get_barrier_semaphore()
    greeted = [by_high(k) for k in range(1, high)] + [by_core, by_mid]
    greeted += [by_part(k) for k in range(1, parts)]
    for device in greeted:
        pl.semaphore_signal(barrier, inc=1, device_id=device, device_id_type=pl.DeviceIdType.MESH)

    loads = [
        pltpu.make_async_copy(src, dst, sem_in.at[n])
        for n, (src, dst) in enumerate(
            [(qw_hbm, qw_ref), (qx_hbm, qx_ref), (iw_hbm, iw_ref), (ix_hbm, ix_ref)]
        )
    ]
    for load in loads:
        load.start()

    logq_col = as_column(logq_ref[...])
    count = logq_col.shape[0]
    pieces = []
    for c in range(rows // LANES):
        lane = slice(c * LANES, (c + 1) * LANES)
        bucket = lax.broadcasted_iota(jnp.int32, (count, LANES), 0)
        chosen = jnp.where(bucket == buckets_ref[:, lane], logq_col, 0.0)
        pieces.append(jnp.sum(chosen, axis=0, keepdims=True))
    meta_q[0, 0:1, :] = ids_ref[...].astype(F32)
    meta_q[0, 1:2, :] = jnp.concatenate(pieces, axis=1)
    meta_q[0, 2:8, :] = jnp.zeros((6, rows), F32)
    meta_i[0] = meta_q[0]
    loads[0].wait()
    loads[1].wait()
    q_all[0] = matmul(qx_ref[...], qw_ref[...]).astype(BF16)
    pl.semaphore_wait(barrier, len(greeted))

    copies_q, copies_m, copies_i, copies_n = [], [], [], []
    for k in range(1, high):
        copies_q.append(send(q_all.at[0], q_all.at[k], sem_qs.at[k], sem_qr.at[k], by_high(k)))
        copies_m.append(send(meta_q.at[0], meta_q.at[k], sem_ms.at[k], sem_mr.at[k], by_high(k)))
    loads[2].wait()
    loads[3].wait()
    i_all[0] = matmul(ix_ref[...], iw_ref[...]).astype(BF16)
    near = [None, by_core, by_mid, by_core]
    copies_n = [None] * LOW
    copies_i = [None] * LOW

    def spread(source, slot):
        copies_n[slot] = send(
            meta_i.at[source], meta_i.at[slot], sem_ns.at[slot], sem_nr.at[slot], near[slot]
        )
        copies_i[slot] = send(
            i_all.at[source], i_all.at[slot], sem_is.at[slot], sem_ir.at[slot], near[slot]
        )

    spread(0, 2)
    spread(0, 1)

    qx_turned[...] = jnp.transpose(qx_ref[...])
    ix_turned[...] = jnp.transpose(ix_ref[...])

    def prepare(j):
        span = slice(j * rows, (j + 1) * rows)
        i_turned[:, span] = jnp.transpose(i_all[j])
        id_col[span, :] = as_column(meta_i[j, 0:1, :])
        corr_col[span, :] = as_column(meta_i[j, 1:2, :])

    prepare(0)
    lane_chunks = rows // LANES
    copies_o = []
    positive = None
    for k in range(high):
        if k:
            copies_q[k - 1].wait_recv()
            copies_m[k - 1].wait_recv()
        id_row = meta_q[k, 0:1, :]
        peaks = [jnp.full((8, LANES), EXCLUDED, F32)] * lane_chunks
        for j in range(LOW):
            if k == 0 and j:
                copies_i[j].wait_recv()
                copies_n[j].wait_recv()
                if j == 2:
                    spread(2, 3)
                prepare(j)
            span = slice(j * rows, (j + 1) * rows)
            raw = contract_last(i_all[j], q_all[k])
            if k == 0 and j == 0:
                row = lax.broadcasted_iota(jnp.int32, (rows, LANES), 0)
                col = lax.broadcasted_iota(jnp.int32, (rows, LANES), 1)
                diag = []
            for c in range(lane_chunks):
                lane = slice(c * LANES, (c + 1) * LANES)
                value = raw[:, lane] * scaling - corr_col[span, :]
                same = id_col[span, :] == id_row[:, lane]
                if k == 0 and j == 0:
                    on_diag = row == col + c * LANES
                    diag.append(jnp.sum(jnp.where(on_diag, value, 0.0), axis=0, keepdims=True))
                    same = same & jnp.logical_not(on_diag)
                value = jnp.where(same, EXCLUDED, value)
                score[span, lane] = value
                peaks[c] = jnp.maximum(peaks[c], jnp.max(value.reshape(rows // 8, 8, LANES), axis=0))
            if k == 0 and j == 0:
                positive = jnp.concatenate(diag, axis=1)
        peak = jnp.max(jnp.concatenate(peaks, axis=1), axis=0, keepdims=True)
        total = jnp.zeros((8, rows), F32)
        for j in range(LOW):
            span = slice(j * rows, (j + 1) * rows)
            value = jnp.exp(score[span, :] - peak)
            weight[span, k * rows:(k + 1) * rows] = value.astype(BF16)
            total += jnp.sum(value.reshape(rows // 8, 8, rows), axis=0)
        stats[0, 2 * k:2 * k + 1, :] = peak
        stats[0, 2 * k + 1:2 * k + 2, :] = jnp.sum(total, axis=0, keepdims=True)
        partial = matmul(i_turned[...], weight[:, k * rows:(k + 1) * rows])
        if k == 0:
            o_own[...] = partial
        else:
            o_send[k] = partial.astype(BF16)
            copies_o.append(
                send(o_send.at[k], o_recv.at[k], sem_os.at[k], sem_or.at[k], by_high(high - k))
            )

    copies_s = [
        send(stats.at[0], stats.at[k], sem_ss.at[k], sem_sr.at[k], by_high(k)) for k in range(1, high)
    ]
    for copy in copies_s:
        copy.wait_recv()
    log_total = []
    for k in range(high):
        peaks = [stats[d, 2 * ((k - d) % high):2 * ((k - d) % high) + 1, :] for d in range(high)]
        sums = [stats[d, 2 * ((k - d) % high) + 1:2 * ((k - d) % high) + 2, :] for d in range(high)]
        top = functools.reduce(jnp.maximum, peaks)
        whole = functools.reduce(jnp.add, [s * jnp.exp(p - top) for p, s in zip(peaks, sums)])
        log_total.append(top + jnp.log(whole))
        factor = jnp.exp(peaks[0] - log_total[k])
        q_scaled[k * rows:(k + 1) * rows, :] = (
            q_all[k].astype(F32) * as_wide_column(factor, embed)
        ).astype(BF16)

    def item_sums(j):
        return matmul(weight[j * rows:(j + 1) * rows, :], q_scaled[...])

    copies_u = [None] * LOW
    for j in (3, 1):
        u_send[j] = item_sums(j).astype(BF16)
        copies_u[j] = send(u_send.at[j], u_recv.at[j], sem_us.at[j], sem_ur.at[j], by_core)
    u_far[...] = item_sums(2)
    copies_u[3].wait_recv()
    u_send[2] = (u_far[...] + u_recv[3].astype(F32)).astype(BF16)
    copies_u[2] = send(u_send.at[2], u_recv.at[2], sem_us.at[2], sem_ur.at[2], by_mid)
    u_own[...] = item_sums(0)

    own_total = o_own[...] * jnp.exp(stats[0, 0:1, :] - log_total[0])
    for k in range(1, high):
        copies_o[k - 1].wait_recv()
        d = high - k
        own_total += o_recv[k].astype(F32) * jnp.exp(stats[d, 2 * k:2 * k + 1, :] - log_total[0])
    query_grad = ((jnp.transpose(own_total) - i_all[0].astype(F32)) * scaling).astype(BF16)
    grads[0] = matmul(qx_turned[...], query_grad)
    lost = jnp.sum(log_total[0] - positive, axis=1, keepdims=True)

    sums = u_own[...]
    for j in (1, 2):
        copies_u[j].wait_recv()
        sums += u_recv[j].astype(F32)
    item_grad = ((sums - q_all[0].astype(F32)) * scaling).astype(BF16)
    grads[1] = matmul(ix_turned[...], item_grad)

    pending = copies_q + copies_m + copies_i[1:] + copies_n[1:] + copies_o + copies_s + copies_u[1:]

    loss_buf[0] = jnp.broadcast_to(lost, (8, LANES))
    slot = 0

    def loss_round(partners):
        nonlocal slot
        base, copies = slot, []
        for n, device in enumerate(partners):
            at = base + 1 + n
            copies.append(send(loss_buf.at[base], loss_buf.at[at], sem_ls.at[at], sem_lr.at[at], device))
        return base, copies

    def loss_sum(base, copies):
        nonlocal slot
        value = loss_buf[base]
        for n, copy in enumerate(copies):
            copy.wait_recv()
            value += loss_buf[base + 1 + n]
        pending.extend(copies)
        slot = base + 1 + len(copies)
        loss_buf[slot] = value

    copy = send(grads.at[1 - core], half_recv, sem_hs.at[0], sem_hr.at[0], by_core)
    base, copies = loss_round([by_core])
    copy.wait_recv()
    acc[...] = (grads[core] + half_recv[...]).reshape(acc.shape)
    pending.append(copy)
    loss_sum(base, copies)
    base, copies = loss_round([by_part(k) for k in range(1, parts)])

    @pl.when(core == 0)
    def _():
        moved = []
        for k in range(1, parts):
            send1[k] = acc[lax.rem(part + k, parts)].astype(BF16)
            moved.append(send(send1.at[k], recv1.at[k], sem_1s.at[k], sem_1r.at[k], by_part(k)))
        value = acc[part]
        for k in range(1, parts):
            moved[k - 1].wait_recv()
            value += recv1[k].astype(F32)
        acc1[...] = value
        send2[...] = acc1[1 - mid].astype(BF16)
        moved.append(send(send2, recv2, sem_2s.at[0], sem_2r.at[0], by_mid))
        moved[-1].wait_recv()
        acc2[...] = acc1[mid] + recv2[...].astype(F32)
        for copy in moved:
            copy.wait_send()

    @pl.when(core == 1)
    def _():
        for k in range(parts):
            sendb[k] = acc[k, 1 - mid].astype(BF16)
        moved = [send(sendb, recvb, sem_bs.at[0], sem_br.at[0], by_mid)]
        moved[0].wait_recv()
        for k in range(parts):
            accb[k] = acc[k, mid] + recvb[k].astype(F32)
        for k in range(1, parts):
            sendc[k] = accb[lax.rem(part + k, parts)].astype(BF16)
            moved.append(send(sendc.at[k], recvc.at[k], sem_cs.at[k], sem_cr.at[k], by_part(k)))
        value = accb[part]
        for k in range(1, parts):
            moved[k].wait_recv()
            value += recvc[k].astype(F32)
        acc2[...] = value
        for copy in moved:
            copy.wait_send()

    loss_sum(base, copies)
    base, copies = loss_round([by_mid])
    moved = []
    for k in range(1, high):
        send3[k] = acc2[lax.rem(hi + k, high)].astype(BF16)
        moved.append(send(send3.at[k], recv3.at[k], sem_3s.at[k], sem_3r.at[k], by_high(k)))
    value = acc2[hi]
    for k in range(1, high):
        moved[k - 1].wait_recv()
        value += recv3[k].astype(F32)
    full[core, part, mid, hi] = value.astype(BF16)
    pending.extend(moved)
    loss_sum(base, copies)

    place = full.at[core, part, mid, hi]
    moved = [send(place, place, sem_g3s.at[k], sem_g3r.at[k], by_high(k)) for k in range(1, high)]
    base, copies = loss_round([by_high(k) for k in range(1, high)])
    for copy in moved:
        copy.wait_recv()
    pending.extend(moved)

    @pl.when(core == 0)
    def _():
        place = full.at[core, part, mid]
        moved = [send(place, place, sem_g2s.at[0], sem_g2r.at[0], by_mid)]
        moved[0].wait_recv()
        place = full.at[core, part]
        for k in range(1, parts):
            moved.append(send(place, place, sem_g1s.at[k], sem_g1r.at[k], by_part(k)))
        for copy in moved[1:]:
            copy.wait_recv()
        for copy in moved:
            copy.wait_send()

    @pl.when(core == 1)
    def _():
        place = full.at[core, part, mid]
        first = [send(place, place, sem_g1s.at[k], sem_g1r.at[k], by_part(k)) for k in range(1, parts)]
        for copy in first:
            copy.wait_recv()
        second = []
        for k in range(parts):
            place = full.at[core, k, mid]
            second.append(send(place, place, sem_g2s.at[k], sem_g2r.at[k], by_mid))
        for copy in second:
            copy.wait_recv()
        for copy in first + second:
            copy.wait_send()

    place = full.at[core]
    copy = send(place, place, sem_g0s.at[0], sem_g0r.at[0], by_core)
    own_out = pltpu.make_async_copy(place, grad_ref.at[core], sem_out.at[0])
    own_out.start()
    loss_sum(base, copies)
    loss_ref[...] = loss_buf[slot, 0:1, 0:1] * (1.0 / (parts * high * LOW * rows))
    copy.wait_recv()
    pending.append(copy)
    other_out = pltpu.make_async_copy(full.at[1 - core], grad_ref.at[1 - core], sem_out.at[1])
    other_out.start()
    for copy in pending:
        copy.wait_send()
    own_out.wait()
    other_out.wait()


def on_device(high, parts, query_feats, item_feats, item_ids, bucket_ids, bucket_logq, query_tower, item_tower):
    rows, width = query_feats.shape[1:]
    embed = query_tower.shape[1]
    items = LOW * rows
    stat_rows = -(-2 * high // 8) * 8
    rounds = 1 + 1 + 1 + (parts - 1) + 1 + 1 + 1 + (high - 1) + 1
    r3 = width // (2 * parts * high)
    vmem, dma = pltpu.VMEM, pltpu.SemaphoreType.DMA
    block = (rows, embed)
    far = (2, high, r3, embed)
    wide = (parts, high, r3, embed)
    scratch = [
        vmem((rows, width), BF16), vmem((rows, width), BF16),
        vmem((width, embed), BF16), vmem((width, embed), BF16),
        vmem((high,) + block, BF16), vmem((LOW,) + block, BF16),
        vmem((high, 8, rows), F32), vmem((LOW, 8, rows), F32),
        vmem((embed, items), BF16), vmem((width, rows), BF16), vmem((width, rows), BF16),
        vmem((items, LANES), F32), vmem((items, LANES), F32),
        vmem((items, rows), F32), vmem((items, high * rows), BF16), vmem((high * rows, embed), BF16),
        vmem((high, stat_rows, rows), F32),
        vmem((high, embed, rows), BF16), vmem((high, embed, rows), BF16), vmem((embed, rows), F32),
        vmem((LOW,) + block, BF16), vmem((LOW,) + block, BF16), vmem(block, F32), vmem(block, F32),
        vmem((2, width, embed), F32), vmem((width, embed), F32), vmem((parts,) + far, F32),
        vmem((parts,) + far, BF16), vmem((parts,) + far, BF16), vmem(far, F32),
        vmem(far[1:], BF16), vmem(far[1:], BF16), vmem(far[1:], F32),
        vmem((high, r3, embed), BF16), vmem((high, r3, embed), BF16),
        vmem(wide, BF16), vmem(wide, BF16), vmem(wide, F32), vmem(wide, BF16), vmem(wide, BF16),
        vmem((2, parts) + far, BF16), vmem((rounds, 8, LANES), F32),
    ]
    scratch += [dma((n,)) for n in (4, 2)]
    scratch += [dma((n,)) for n in (high, high, LOW, LOW, high, high, LOW, LOW)]
    scratch += [dma((n,)) for n in (high, high, high, high, LOW, LOW)]
    scratch += [dma((n,)) for n in (1, 1, parts, parts, 1, 1, high, high)]
    scratch += [dma((n,)) for n in (1, 1, parts, parts)]
    scratch += [dma((n,)) for n in (rounds, rounds, high, high, parts, parts, parts, parts, 1, 1)]
    space = pltpu.VMEM
    grad, loss = pl.pallas_call(
        functools.partial(kernel, high, parts),
        out_shape=(
            jax.ShapeDtypeStruct((2, parts) + far, BF16),
            jax.ShapeDtypeStruct((1, 1), F32),
        ),
        in_specs=[
            pl.BlockSpec(memory_space=space)
            for space in (pl.ANY, pl.ANY, space, space, space, pl.ANY, pl.ANY)
        ],
        out_specs=(pl.BlockSpec(memory_space=pl.ANY), pl.BlockSpec(memory_space=space)),
        scratch_shapes=scratch,
        compiler_params=pltpu.CompilerParams(
            collective_id=0, has_side_effects=True, vmem_limit_bytes=60 * 1024 * 1024
        ),
        name="two_tower",
    )(
        query_feats[0], item_feats[0], item_ids, bucket_ids, bucket_logq[None, :], query_tower, item_tower
    )
    grad = grad.reshape(2, width, embed).astype(F32)
    return grad[0], grad[1], loss.reshape(())


def solution(mesh):
    high = mesh.shape["blk"] // LOW
    return jax.shard_map(
        functools.partial(on_device, high, mesh.shape["dp"]),
        mesh=mesh,
        in_specs=(
            P("dp", "blk", None), P("dp", "blk", None), P("dp", "blk"), P("dp", "blk"), P(), P(), P(),
        ),
        out_specs=(P(), P(), P()),
        check_vma=False,
    )
```

```python
import functools
import math

import jax
import jax.numpy as jnp
from jax import lax
from jax.experimental import pallas as pl
from jax.experimental.pallas import tpu as pltpu
from jax.sharding import PartitionSpec as P

EXCLUDED = -1e30
LANES = 128
LOW = 4
F32 = jnp.float32
BF16 = jnp.bfloat16


def contract_last(left, right):
    return lax.dot_general(left, right, (((1,), (1,)), ((), ())), preferred_element_type=F32)


def matmul(left, right):
    return jnp.dot(left, right, preferred_element_type=F32)


def as_column(row):
    return jnp.transpose(jnp.broadcast_to(row, (LANES, row.shape[1])))


def as_wide_column(row, width):
    column = as_column(row)
    return jnp.concatenate([column] * (width // LANES), axis=1)


def kernel(
    high, parts,
    qx_hbm, ix_hbm, ids_ref, buckets_ref, logq_ref, qw_hbm, iw_hbm,
    grad_ref, loss_ref,
    qx_ref, ix_ref, qw_ref, iw_ref,
    q_all, i_all, meta_q, meta_i, i_turned, qx_turned, ix_turned,
    id_col, corr_col, score, weight, q_scaled,
    stats, o_send, o_recv, o_own, u_send, u_recv, u_own, u_far,
    grads, half_recv, acc, acc2, send3, recv3,
    sendb, recvb, accb, sendc, recvc, full, loss_buf,
    sem_in, sem_out,
    sem_qs, sem_qr, sem_is, sem_ir, sem_ms, sem_mr, sem_ns, sem_nr,
    sem_ss, sem_sr, sem_os, sem_or, sem_us, sem_ur,
    sem_hs, sem_hr, sem_3s, sem_3r,
    sem_bs, sem_br, sem_cs, sem_cr,
    sem_ls, sem_lr, sem_g3s, sem_g3r, sem_g2s, sem_g2r, sem_g1s, sem_g1r, sem_g0s, sem_g0r,
):
    rows, width = qx_ref.shape
    embed = qw_ref.shape[1]
    scaling = 1.0 / math.sqrt(embed)
    me = lax.axis_index("blk")
    part = lax.axis_index("dp")
    hi, lo = me // LOW, me % LOW
    mid, core = lo // 2, lo % 2

    def by_high(k):
        return {"blk": lax.rem(hi + k, high) * LOW + lo}

    def by_part(k):
        return {"dp": lax.rem(part + k, parts)}

    by_core = {"blk": hi * LOW + mid * 2 + (1 - core)}
    by_mid = {"blk": hi * LOW + (1 - mid) * 2 + core}

    def send(src, dst, send_sem, recv_sem, device):
        copy = pltpu.make_async_remote_copy(
            src_ref=src, dst_ref=dst, send_sem=send_sem, recv_sem=recv_sem,
            device_id=device, device_id_type=pl.DeviceIdType.MESH,
        )
        copy.start()
        return copy

    barrier = pltpu.get_barrier_semaphore()
    greeted = [by_high(k) for k in range(1, high)] + [by_core, by_mid]
    greeted += [by_part(k) for k in range(1, parts)]
    for device in greeted:
        pl.semaphore_signal(barrier, inc=1, device_id=device, device_id_type=pl.DeviceIdType.MESH)

    loads = [
        pltpu.make_async_copy(src, dst, sem_in.at[n])
        for n, (src, dst) in enumerate(
            [(qw_hbm, qw_ref), (qx_hbm, qx_ref), (iw_hbm, iw_ref), (ix_hbm, ix_ref)]
        )
    ]
    for load in loads:
        load.start()

    logq_col = as_column(logq_ref[...])
    count = logq_col.shape[0]
    pieces = []
    for c in range(rows // LANES):
        lane = slice(c * LANES, (c + 1) * LANES)
        bucket = lax.broadcasted_iota(jnp.int32, (count, LANES), 0)
        chosen = jnp.where(bucket == buckets_ref[:, lane], logq_col, 0.0)
        pieces.append(jnp.sum(chosen, axis=0, keepdims=True))
    meta_q[0, 0:1, :] = ids_ref[...].astype(F32)
    meta_q[0, 1:2, :] = jnp.concatenate(pieces, axis=1)
    meta_q[0, 2:8, :] = jnp.zeros((6, rows), F32)
    meta_i[0] = meta_q[0]
    loads[0].wait()
    loads[1].wait()
    q_all[0] = matmul(qx_ref[...], qw_ref[...]).astype(BF16)
    pl.semaphore_wait(barrier, len(greeted))

    copies_q, copies_m, copies_i, copies_n = [], [], [], []
    for k in range(1, high):
        copies_q.append(send(q_all.at[0], q_all.at[k], sem_qs.at[k], sem_qr.at[k], by_high(k)))
        copies_m.append(send(meta_q.at[0], meta_q.at[k], sem_ms.at[k], sem_mr.at[k], by_high(k)))
    loads[2].wait()
    loads[3].wait()
    i_all[0] = matmul(ix_ref[...], iw_ref[...]).astype(BF16)
    near = [None, by_core, by_mid, by_core]
    copies_n = [None] * LOW
    copies_i = [None] * LOW

    def spread(source, slot):
        copies_n[slot] = send(
            meta_i.at[source], meta_i.at[slot], sem_ns.at[slot], sem_nr.at[slot], near[slot]
        )
        copies_i[slot] = send(
            i_all.at[source], i_all.at[slot], sem_is.at[slot], sem_ir.at[slot], near[slot]
        )

    spread(0, 2)
    spread(0, 1)

    qx_turned[...] = jnp.transpose(qx_ref[...])
    ix_turned[...] = jnp.transpose(ix_ref[...])

    def prepare(j):
        span = slice(j * rows, (j + 1) * rows)
        i_turned[:, span] = jnp.transpose(i_all[j])
        id_col[span, :] = as_column(meta_i[j, 0:1, :])
        corr_col[span, :] = as_column(meta_i[j, 1:2, :])

    prepare(0)
    lane_chunks = rows // LANES
    copies_o = []
    positive = None
    for k in range(high):
        if k:
            copies_q[k - 1].wait_recv()
            copies_m[k - 1].wait_recv()
        id_row = meta_q[k, 0:1, :]
        peaks = [jnp.full((8, LANES), EXCLUDED, F32)] * lane_chunks
        for j in range(LOW):
            if k == 0 and j:
                copies_i[j].wait_recv()
                copies_n[j].wait_recv()
                if j == 2:
                    spread(2, 3)
                prepare(j)
            span = slice(j * rows, (j + 1) * rows)
            raw = contract_last(i_all[j], q_all[k])
            if k == 0 and j == 0:
                row = lax.broadcasted_iota(jnp.int32, (rows, LANES), 0)
                col = lax.broadcasted_iota(jnp.int32, (rows, LANES), 1)
                diag = []
            for c in range(lane_chunks):
                lane = slice(c * LANES, (c + 1) * LANES)
                value = raw[:, lane] * scaling - corr_col[span, :]
                same = id_col[span, :] == id_row[:, lane]
                if k == 0 and j == 0:
                    on_diag = row == col + c * LANES
                    diag.append(jnp.sum(jnp.where(on_diag, value, 0.0), axis=0, keepdims=True))
                    same = same & jnp.logical_not(on_diag)
                value = jnp.where(same, EXCLUDED, value)
                score[span, lane] = value
                peaks[c] = jnp.maximum(peaks[c], jnp.max(value.reshape(rows // 8, 8, LANES), axis=0))
            if k == 0 and j == 0:
                positive = jnp.concatenate(diag, axis=1)
        peak = jnp.max(jnp.concatenate(peaks, axis=1), axis=0, keepdims=True)
        total = jnp.zeros((8, rows), F32)
        for j in range(LOW):
            span = slice(j * rows, (j + 1) * rows)
            value = jnp.exp(score[span, :] - peak)
            weight[span, k * rows:(k + 1) * rows] = value.astype(BF16)
            total += jnp.sum(value.reshape(rows // 8, 8, rows), axis=0)
        stats[0, 2 * k:2 * k + 1, :] = peak
        stats[0, 2 * k + 1:2 * k + 2, :] = jnp.sum(total, axis=0, keepdims=True)
        partial = matmul(i_turned[...], weight[:, k * rows:(k + 1) * rows])
        if k == 0:
            o_own[...] = partial
        else:
            o_send[k] = partial.astype(BF16)

    copies_s = [
        send(stats.at[0], stats.at[k], sem_ss.at[k], sem_sr.at[k], by_high(k)) for k in range(1, high)
    ]
    for k in range(1, high):
        copies_o.append(
            send(o_send.at[k], o_recv.at[k], sem_os.at[k], sem_or.at[k], by_high(high - k))
        )
    for copy in copies_s:
        copy.wait_recv()
    log_total = []
    for k in range(high):
        peaks = [stats[d, 2 * ((k - d) % high):2 * ((k - d) % high) + 1, :] for d in range(high)]
        sums = [stats[d, 2 * ((k - d) % high) + 1:2 * ((k - d) % high) + 2, :] for d in range(high)]
        top = functools.reduce(jnp.maximum, peaks)
        whole = functools.reduce(jnp.add, [s * jnp.exp(p - top) for p, s in zip(peaks, sums)])
        log_total.append(top + jnp.log(whole))
        factor = jnp.exp(peaks[0] - log_total[k])
        q_scaled[k * rows:(k + 1) * rows, :] = (
            q_all[k].astype(F32) * as_wide_column(factor, embed)
        ).astype(BF16)

    def item_sums(j):
        return matmul(weight[j * rows:(j + 1) * rows, :], q_scaled[...])

    copies_u = [None] * LOW
    for j in (3, 1):
        u_send[j] = item_sums(j).astype(BF16)
        copies_u[j] = send(u_send.at[j], u_recv.at[j], sem_us.at[j], sem_ur.at[j], by_core)
    u_far[...] = item_sums(2)
    copies_u[3].wait_recv()
    u_send[2] = (u_far[...] + u_recv[3].astype(F32)).astype(BF16)
    copies_u[2] = send(u_send.at[2], u_recv.at[2], sem_us.at[2], sem_ur.at[2], by_mid)
    u_own[...] = item_sums(0)

    sums = u_own[...]
    for j in (1, 2):
        copies_u[j].wait_recv()
        sums += u_recv[j].astype(F32)
    item_grad = ((sums - q_all[0].astype(F32)) * scaling).astype(BF16)
    grads[1] = matmul(ix_turned[...], item_grad)

    own_total = o_own[...] * jnp.exp(stats[0, 0:1, :] - log_total[0])
    for k in range(1, high):
        copies_o[k - 1].wait_recv()
        d = high - k
        own_total += o_recv[k].astype(F32) * jnp.exp(stats[d, 2 * k:2 * k + 1, :] - log_total[0])
    query_grad = ((jnp.transpose(own_total) - i_all[0].astype(F32)) * scaling).astype(BF16)
    grads[0] = matmul(qx_turned[...], query_grad)
    lost = jnp.sum(log_total[0] - positive, axis=1, keepdims=True)

    pending = copies_q + copies_m + copies_i[1:] + copies_n[1:] + copies_o + copies_s + copies_u[1:]

    loss_buf[0] = jnp.broadcast_to(lost, (8, LANES))
    slot = 0

    def loss_round(partners):
        nonlocal slot
        base, copies = slot, []
        for n, device in enumerate(partners):
            at = base + 1 + n
            copies.append(send(loss_buf.at[base], loss_buf.at[at], sem_ls.at[at], sem_lr.at[at], device))
        return base, copies

    def loss_sum(base, copies):
        nonlocal slot
        value = loss_buf[base]
        for n, copy in enumerate(copies):
            copy.wait_recv()
            value += loss_buf[base + 1 + n]
        pending.extend(copies)
        slot = base + 1 + len(copies)
        loss_buf[slot] = value

    copy = send(grads.at[1 - core], half_recv, sem_hs.at[0], sem_hr.at[0], by_core)
    base, copies = loss_round([by_core])
    copy.wait_recv()
    acc[...] = (grads[core] + half_recv[...]).reshape(acc.shape)
    pending.append(copy)
    loss_sum(base, copies)
    base, copies = loss_round([by_mid])
    for k in range(parts):
        sendb[k] = acc[k, 1 - mid].astype(BF16)
    copy = send(sendb, recvb, sem_bs.at[0], sem_br.at[0], by_mid)
    copy.wait_recv()
    pending.append(copy)
    for k in range(parts):
        accb[k] = acc[k, mid] + recvb[k].astype(F32)
    loss_sum(base, copies)
    base, copies = loss_round([by_part(k) for k in range(1, parts)])
    moved = []
    for k in range(1, parts):
        sendc[k] = accb[lax.rem(part + k, parts)].astype(BF16)
        moved.append(send(sendc.at[k], recvc.at[k], sem_cs.at[k], sem_cr.at[k], by_part(k)))
    value = accb[part]
    for k in range(1, parts):
        moved[k - 1].wait_recv()
        value += recvc[k].astype(F32)
    acc2[...] = value
    pending.extend(moved)

    moved = []
    for k in range(1, high):
        send3[k] = acc2[lax.rem(hi + k, high)].astype(BF16)
        moved.append(send(send3.at[k], recv3.at[k], sem_3s.at[k], sem_3r.at[k], by_high(k)))
    value = acc2[hi]
    for k in range(1, high):
        moved[k - 1].wait_recv()
        value += recv3[k].astype(F32)
    full[core, part, mid, hi] = value.astype(BF16)
    pending.extend(moved)
    loss_sum(base, copies)

    place = full.at[core, part, mid, hi]
    moved = [send(place, place, sem_g3s.at[k], sem_g3r.at[k], by_high(k)) for k in range(1, high)]
    base, copies = loss_round([by_high(k) for k in range(1, high)])
    for copy in moved:
        copy.wait_recv()
    pending.extend(moved)

    place = full.at[core, part, mid]
    moved = [send(place, place, sem_g1s.at[k], sem_g1r.at[k], by_part(k)) for k in range(1, parts)]
    for copy in moved:
        copy.wait_recv()
    pending.extend(moved)
    moved = []
    for k in range(parts):
        place = full.at[core, k, mid]
        moved.append(send(place, place, sem_g2s.at[k], sem_g2r.at[k], by_mid))
    for copy in moved:
        copy.wait_recv()
    pending.extend(moved)
    place = full.at[core]
    copy = send(place, place, sem_g0s.at[0], sem_g0r.at[0], by_core)
    own_out = pltpu.make_async_copy(place, grad_ref.at[core], sem_out.at[0])
    own_out.start()
    loss_sum(base, copies)
    loss_ref[...] = loss_buf[slot, 0:1, 0:1] * (1.0 / (parts * high * LOW * rows))
    copy.wait_recv()
    pending.append(copy)
    other_out = pltpu.make_async_copy(full.at[1 - core], grad_ref.at[1 - core], sem_out.at[1])
    other_out.start()
    for copy in pending:
        copy.wait_send()
    own_out.wait()
    other_out.wait()


def on_device(high, parts, query_feats, item_feats, item_ids, bucket_ids, bucket_logq, query_tower, item_tower):
    rows, width = query_feats.shape[1:]
    embed = query_tower.shape[1]
    items = LOW * rows
    stat_rows = -(-2 * high // 8) * 8
    rounds = 1 + 1 + 1 + (parts - 1) + 1 + 1 + 1 + (high - 1) + 1
    r3 = width // (2 * parts * high)
    vmem, dma = pltpu.VMEM, pltpu.SemaphoreType.DMA
    block = (rows, embed)
    far = (2, high, r3, embed)
    wide = (parts, high, r3, embed)
    scratch = [
        vmem((rows, width), BF16), vmem((rows, width), BF16),
        vmem((width, embed), BF16), vmem((width, embed), BF16),
        vmem((high,) + block, BF16), vmem((LOW,) + block, BF16),
        vmem((high, 8, rows), F32), vmem((LOW, 8, rows), F32),
        vmem((embed, items), BF16), vmem((width, rows), BF16), vmem((width, rows), BF16),
        vmem((items, LANES), F32), vmem((items, LANES), F32),
        vmem((items, rows), F32), vmem((items, high * rows), BF16), vmem((high * rows, embed), BF16),
        vmem((high, stat_rows, rows), F32),
        vmem((high, embed, rows), BF16), vmem((high, embed, rows), BF16), vmem((embed, rows), F32),
        vmem((LOW,) + block, BF16), vmem((LOW,) + block, BF16), vmem(block, F32), vmem(block, F32),
        vmem((2, width, embed), F32), vmem((width, embed), F32), vmem((parts,) + far, F32),
        vmem(far[1:], F32),
        vmem((high, r3, embed), BF16), vmem((high, r3, embed), BF16),
        vmem(wide, BF16), vmem(wide, BF16), vmem(wide, F32), vmem(wide, BF16), vmem(wide, BF16),
        vmem((2, parts) + far, BF16), vmem((rounds, 8, LANES), F32),
    ]
    scratch += [dma((n,)) for n in (4, 2)]
    scratch += [dma((n,)) for n in (high, high, LOW, LOW, high, high, LOW, LOW)]
    scratch += [dma((n,)) for n in (high, high, high, high, LOW, LOW)]
    scratch += [dma((n,)) for n in (1, 1, high, high)]
    scratch += [dma((n,)) for n in (1, 1, parts, parts)]
    scratch += [dma((n,)) for n in (rounds, rounds, high, high, parts, parts, parts, parts, 1, 1)]
    space = pltpu.VMEM
    grad, loss = pl.pallas_call(
        functools.partial(kernel, high, parts),
        out_shape=(
            jax.ShapeDtypeStruct((2, parts) + far, BF16),
            jax.ShapeDtypeStruct((1, 1), F32),
        ),
        in_specs=[
            pl.BlockSpec(memory_space=space)
            for space in (pl.ANY, pl.ANY, space, space, space, pl.ANY, pl.ANY)
        ],
        out_specs=(pl.BlockSpec(memory_space=pl.ANY), pl.BlockSpec(memory_space=space)),
        scratch_shapes=scratch,
        compiler_params=pltpu.CompilerParams(
            collective_id=0, has_side_effects=True, vmem_limit_bytes=60 * 1024 * 1024
        ),
        name="two_tower",
    )(
        query_feats[0], item_feats[0], item_ids, bucket_ids, bucket_logq[None, :], query_tower, item_tower
    )
    grad = grad.reshape(2, width, embed).astype(F32)
    return grad[0], grad[1], loss.reshape(())


def solution(mesh):
    high = mesh.shape["blk"] // LOW
    return jax.shard_map(
        functools.partial(on_device, high, mesh.shape["dp"]),
        mesh=mesh,
        in_specs=(
            P("dp", "blk", None), P("dp", "blk", None), P("dp", "blk"), P("dp", "blk"), P(), P(), P(),
        ),
        out_specs=(P(), P(), P()),
        check_vma=False,
    )
```

```python
import functools
import math

import jax
import jax.numpy as jnp
from jax import lax
from jax.experimental import pallas as pl
from jax.experimental.pallas import tpu as pltpu
from jax.sharding import PartitionSpec as P

EXCLUDED = -1e30
LANES = 128
LOW = 4
F32 = jnp.float32
BF16 = jnp.bfloat16


def contract_last(left, right):
    return lax.dot_general(left, right, (((1,), (1,)), ((), ())), preferred_element_type=F32)


def matmul(left, right):
    return jnp.dot(left, right, preferred_element_type=F32)


def as_column(row):
    return jnp.transpose(jnp.broadcast_to(row, (LANES, row.shape[1])))


def as_wide_column(row, width):
    column = as_column(row)
    return jnp.concatenate([column] * (width // LANES), axis=1)


def kernel(
    high, parts,
    qx_hbm, ix_hbm, ids_ref, buckets_ref, logq_ref, qw_hbm, iw_hbm,
    grad_ref, loss_ref,
    qx_ref, ix_ref, qw_ref, iw_ref,
    q_all, i_all, meta_q, meta_i, i_turned, qx_turned, ix_turned,
    id_col, corr_col, score, weight, q_scaled,
    stats, o_send, o_recv, o_own, u_send, u_recv, u_own, u_far,
    grads, half_recv, acc, send1, recv1, acc1, send2, recv2, acc2, send3, recv3,
    full, loss_buf,
    sem_in, sem_out,
    sem_qs, sem_qr, sem_is, sem_ir, sem_ms, sem_mr, sem_ns, sem_nr,
    sem_ss, sem_sr, sem_os, sem_or, sem_us, sem_ur,
    sem_hs, sem_hr, sem_1s, sem_1r, sem_2s, sem_2r, sem_3s, sem_3r,
    sem_ls, sem_lr, sem_g3s, sem_g3r, sem_g2s, sem_g2r, sem_g1s, sem_g1r, sem_g0s, sem_g0r,
):
    rows, width = qx_ref.shape
    embed = qw_ref.shape[1]
    scaling = 1.0 / math.sqrt(embed)
    me = lax.axis_index("blk")
    part = lax.axis_index("dp")
    hi, lo = me // LOW, me % LOW
    mid, core = lo // 2, lo % 2

    def by_high(k):
        return {"blk": lax.rem(hi + k, high) * LOW + lo}

    def by_part(k):
        return {"dp": lax.rem(part + k, parts)}

    by_core = {"blk": hi * LOW + mid * 2 + (1 - core)}
    by_mid = {"blk": hi * LOW + (1 - mid) * 2 + core}

    def send(src, dst, send_sem, recv_sem, device):
        copy = pltpu.make_async_remote_copy(
            src_ref=src, dst_ref=dst, send_sem=send_sem, recv_sem=recv_sem,
            device_id=device, device_id_type=pl.DeviceIdType.MESH,
        )
        copy.start()
        return copy

    barrier = pltpu.get_barrier_semaphore()
    greeted = [by_high(k) for k in range(1, high)] + [by_core, by_mid]
    greeted += [by_part(k) for k in range(1, parts)]
    for device in greeted:
        pl.semaphore_signal(barrier, inc=1, device_id=device, device_id_type=pl.DeviceIdType.MESH)

    loads = [
        pltpu.make_async_copy(src, dst, sem_in.at[n])
        for n, (src, dst) in enumerate(
            [(qw_hbm, qw_ref), (qx_hbm, qx_ref), (iw_hbm, iw_ref), (ix_hbm, ix_ref)]
        )
    ]
    for load in loads:
        load.start()

    logq_col = as_column(logq_ref[...])
    count = logq_col.shape[0]
    pieces = []
    for c in range(rows // LANES):
        lane = slice(c * LANES, (c + 1) * LANES)
        bucket = lax.broadcasted_iota(jnp.int32, (count, LANES), 0)
        chosen = jnp.where(bucket == buckets_ref[:, lane], logq_col, 0.0)
        pieces.append(jnp.sum(chosen, axis=0, keepdims=True))
    meta_q[0, 0:1, :] = ids_ref[...].astype(F32)
    meta_q[0, 1:2, :] = jnp.concatenate(pieces, axis=1)
    meta_q[0, 2:8, :] = jnp.zeros((6, rows), F32)
    meta_i[0] = meta_q[0]
    loads[0].wait()
    loads[1].wait()
    q_all[0] = matmul(qx_ref[...], qw_ref[...]).astype(BF16)
    pl.semaphore_wait(barrier, len(greeted))

    copies_q, copies_m, copies_i, copies_n = [], [], [], []
    for k in range(1, high):
        copies_q.append(send(q_all.at[0], q_all.at[k], sem_qs.at[k], sem_qr.at[k], by_high(k)))
        copies_m.append(send(meta_q.at[0], meta_q.at[k], sem_ms.at[k], sem_mr.at[k], by_high(k)))
    loads[2].wait()
    loads[3].wait()
    i_all[0] = matmul(ix_ref[...], iw_ref[...]).astype(BF16)
    near = [None, by_core, by_mid, by_core]
    copies_n = [None] * LOW
    copies_i = [None] * LOW

    def spread(source, slot):
        copies_n[slot] = send(
            meta_i.at[source], meta_i.at[slot], sem_ns.at[slot], sem_nr.at[slot], near[slot]
        )
        copies_i[slot] = send(
            i_all.at[source], i_all.at[slot], sem_is.at[slot], sem_ir.at[slot], near[slot]
        )

    spread(0, 2)
    spread(0, 1)

    qx_turned[...] = jnp.transpose(qx_ref[...])
    ix_turned[...] = jnp.transpose(ix_ref[...])

    def prepare(j):
        span = slice(j * rows, (j + 1) * rows)
        i_turned[:, span] = jnp.transpose(i_all[j])
        id_col[span, :] = as_column(meta_i[j, 0:1, :])
        corr_col[span, :] = as_column(meta_i[j, 1:2, :])

    prepare(0)
    lane_chunks = rows // LANES
    copies_o = []
    positive = None
    for k in range(high):
        if k:
            copies_q[k - 1].wait_recv()
            copies_m[k - 1].wait_recv()
        id_row = meta_q[k, 0:1, :]
        peaks = [jnp.full((8, LANES), EXCLUDED, F32)] * lane_chunks
        for j in range(LOW):
            if k == 0 and j:
                copies_i[j].wait_recv()
                copies_n[j].wait_recv()
                if j == 2:
                    spread(2, 3)
                prepare(j)
            span = slice(j * rows, (j + 1) * rows)
            raw = contract_last(i_all[j], q_all[k])
            if k == 0 and j == 0:
                row = lax.broadcasted_iota(jnp.int32, (rows, LANES), 0)
                col = lax.broadcasted_iota(jnp.int32, (rows, LANES), 1)
                diag = []
            for c in range(lane_chunks):
                lane = slice(c * LANES, (c + 1) * LANES)
                value = raw[:, lane] * scaling - corr_col[span, :]
                same = id_col[span, :] == id_row[:, lane]
                if k == 0 and j == 0:
                    on_diag = row == col + c * LANES
                    diag.append(jnp.sum(jnp.where(on_diag, value, 0.0), axis=0, keepdims=True))
                    same = same & jnp.logical_not(on_diag)
                value = jnp.where(same, EXCLUDED, value)
                score[span, lane] = value
                peaks[c] = jnp.maximum(peaks[c], jnp.max(value.reshape(rows // 8, 8, LANES), axis=0))
            if k == 0 and j == 0:
                positive = jnp.concatenate(diag, axis=1)
        peak = jnp.max(jnp.concatenate(peaks, axis=1), axis=0, keepdims=True)
        total = jnp.zeros((8, rows), F32)
        for j in range(LOW):
            span = slice(j * rows, (j + 1) * rows)
            value = jnp.exp(score[span, :] - peak)
            weight[span, k * rows:(k + 1) * rows] = value.astype(BF16)
            total += jnp.sum(value.reshape(rows // 8, 8, rows), axis=0)
        stats[0, 2 * k:2 * k + 1, :] = peak
        stats[0, 2 * k + 1:2 * k + 2, :] = jnp.sum(total, axis=0, keepdims=True)
        partial = matmul(i_turned[...], weight[:, k * rows:(k + 1) * rows])
        if k == 0:
            o_own[...] = partial
        else:
            o_send[k] = partial.astype(BF16)

    copies_s = [
        send(stats.at[0], stats.at[k], sem_ss.at[k], sem_sr.at[k], by_high(k)) for k in range(1, high)
    ]
    for k in range(1, high):
        copies_o.append(
            send(o_send.at[k], o_recv.at[k], sem_os.at[k], sem_or.at[k], by_high(high - k))
        )
    for copy in copies_s:
        copy.wait_recv()
    log_total = []
    for k in range(high):
        peaks = [stats[d, 2 * ((k - d) % high):2 * ((k - d) % high) + 1, :] for d in range(high)]
        sums = [stats[d, 2 * ((k - d) % high) + 1:2 * ((k - d) % high) + 2, :] for d in range(high)]
        top = functools.reduce(jnp.maximum, peaks)
        whole = functools.reduce(jnp.add, [s * jnp.exp(p - top) for p, s in zip(peaks, sums)])
        log_total.append(top + jnp.log(whole))
        factor = jnp.exp(peaks[0] - log_total[k])
        q_scaled[k * rows:(k + 1) * rows, :] = (
            q_all[k].astype(F32) * as_wide_column(factor, embed)
        ).astype(BF16)

    def item_sums(j):
        return matmul(weight[j * rows:(j + 1) * rows, :], q_scaled[...])

    copies_u = [None] * LOW
    for j in (3, 1):
        u_send[j] = item_sums(j).astype(BF16)
        copies_u[j] = send(u_send.at[j], u_recv.at[j], sem_us.at[j], sem_ur.at[j], by_core)
    u_far[...] = item_sums(2)
    copies_u[3].wait_recv()
    u_send[2] = (u_far[...] + u_recv[3].astype(F32)).astype(BF16)
    copies_u[2] = send(u_send.at[2], u_recv.at[2], sem_us.at[2], sem_ur.at[2], by_mid)
    u_own[...] = item_sums(0)

    sums = u_own[...]
    for j in (1, 2):
        copies_u[j].wait_recv()
        sums += u_recv[j].astype(F32)
    item_grad = ((sums - q_all[0].astype(F32)) * scaling).astype(BF16)
    grads[1] = matmul(ix_turned[...], item_grad)

    own_total = o_own[...] * jnp.exp(stats[0, 0:1, :] - log_total[0])
    for k in range(1, high):
        copies_o[k - 1].wait_recv()
        d = high - k
        own_total += o_recv[k].astype(F32) * jnp.exp(stats[d, 2 * k:2 * k + 1, :] - log_total[0])
    query_grad = ((jnp.transpose(own_total) - i_all[0].astype(F32)) * scaling).astype(BF16)
    grads[0] = matmul(qx_turned[...], query_grad)
    lost = jnp.sum(log_total[0] - positive, axis=1, keepdims=True)

    pending = copies_q + copies_m + copies_i[1:] + copies_n[1:] + copies_o + copies_s + copies_u[1:]

    loss_buf[0] = jnp.broadcast_to(lost, (8, LANES))
    slot = 0

    def loss_round(partners):
        nonlocal slot
        base, copies = slot, []
        for n, device in enumerate(partners):
            at = base + 1 + n
            copies.append(send(loss_buf.at[base], loss_buf.at[at], sem_ls.at[at], sem_lr.at[at], device))
        return base, copies

    def loss_sum(base, copies):
        nonlocal slot
        value = loss_buf[base]
        for n, copy in enumerate(copies):
            copy.wait_recv()
            value += loss_buf[base + 1 + n]
        pending.extend(copies)
        slot = base + 1 + len(copies)
        loss_buf[slot] = value

    copy = send(grads.at[1 - core], half_recv, sem_hs.at[0], sem_hr.at[0], by_core)
    base, copies = loss_round([by_core])
    copy.wait_recv()
    acc[...] = (grads[core] + half_recv[...]).reshape(acc.shape)
    pending.append(copy)
    loss_sum(base, copies)
    moved = []
    for k in range(1, parts):
        send1[k] = acc[lax.rem(part + k, parts)].astype(BF16)
        moved.append(send(send1.at[k], recv1.at[k], sem_1s.at[k], sem_1r.at[k], by_part(k)))
    base, copies = loss_round([by_part(k) for k in range(1, parts)])
    value = acc[part]
    for k in range(1, parts):
        moved[k - 1].wait_recv()
        value += recv1[k].astype(F32)
    acc1[...] = value.reshape(acc1.shape)
    pending.extend(moved)
    loss_sum(base, copies)

    send2[...] = acc1[1 - mid].astype(BF16)
    copy = send(send2, recv2, sem_2s.at[0], sem_2r.at[0], by_mid)
    base, copies = loss_round([by_mid])
    copy.wait_recv()
    acc2[...] = (acc1[mid] + recv2[...].astype(F32)).reshape(acc2.shape)
    pending.append(copy)
    loss_sum(base, copies)

    moved = []
    for k in range(1, high):
        send3[k] = acc2[lax.rem(hi + k, high)].astype(BF16)
        moved.append(send(send3.at[k], recv3.at[k], sem_3s.at[k], sem_3r.at[k], by_high(k)))
    value = acc2[hi]
    for k in range(1, high):
        moved[k - 1].wait_recv()
        value += recv3[k].astype(F32)
    full[core, part, mid, hi] = value.astype(BF16)
    pending.extend(moved)

    place = full.at[core, part, mid, hi]
    moved = [send(place, place, sem_g3s.at[k], sem_g3r.at[k], by_high(k)) for k in range(1, high)]
    base, copies = loss_round([by_high(k) for k in range(1, high)])
    for copy in moved:
        copy.wait_recv()
    pending.extend(moved)

    place = full.at[core, part, mid]
    moved = [send(place, place, sem_g1s.at[k], sem_g1r.at[k], by_part(k)) for k in range(1, parts)]
    for copy in moved:
        copy.wait_recv()
    pending.extend(moved)
    moved = []
    for k in range(parts):
        place = full.at[core, k, mid]
        moved.append(send(place, place, sem_g2s.at[k], sem_g2r.at[k], by_mid))
    for copy in moved:
        copy.wait_recv()
    pending.extend(moved)
    place = full.at[core]
    copy = send(place, place, sem_g0s.at[0], sem_g0r.at[0], by_core)
    own_out = pltpu.make_async_copy(place, grad_ref.at[core], sem_out.at[0])
    own_out.start()
    loss_sum(base, copies)
    loss_ref[...] = loss_buf[slot, 0:1, 0:1] * (1.0 / (parts * high * LOW * rows))
    copy.wait_recv()
    pending.append(copy)
    other_out = pltpu.make_async_copy(full.at[1 - core], grad_ref.at[1 - core], sem_out.at[1])
    other_out.start()
    for copy in pending:
        copy.wait_send()
    own_out.wait()
    other_out.wait()


def on_device(high, parts, query_feats, item_feats, item_ids, bucket_ids, bucket_logq, query_tower, item_tower):
    rows, width = query_feats.shape[1:]
    embed = query_tower.shape[1]
    items = LOW * rows
    stat_rows = -(-2 * high // 8) * 8
    rounds = 1 + 1 + 1 + (parts - 1) + 1 + 1 + 1 + (high - 1) + 1
    r3 = width // (2 * parts * high)
    vmem, dma = pltpu.VMEM, pltpu.SemaphoreType.DMA
    block = (rows, embed)
    far = (2, high, r3, embed)
    r1, r2 = width // parts, width // (2 * parts)
    scratch = [
        vmem((rows, width), BF16), vmem((rows, width), BF16),
        vmem((width, embed), BF16), vmem((width, embed), BF16),
        vmem((high,) + block, BF16), vmem((LOW,) + block, BF16),
        vmem((high, 8, rows), F32), vmem((LOW, 8, rows), F32),
        vmem((embed, items), BF16), vmem((width, rows), BF16), vmem((width, rows), BF16),
        vmem((items, LANES), F32), vmem((items, LANES), F32),
        vmem((items, rows), F32), vmem((items, high * rows), BF16), vmem((high * rows, embed), BF16),
        vmem((high, stat_rows, rows), F32),
        vmem((high, embed, rows), BF16), vmem((high, embed, rows), BF16), vmem((embed, rows), F32),
        vmem((LOW,) + block, BF16), vmem((LOW,) + block, BF16), vmem(block, F32), vmem(block, F32),
        vmem((2, width, embed), F32), vmem((width, embed), F32), vmem((parts, r1, embed), F32),
        vmem((parts, r1, embed), BF16), vmem((parts, r1, embed), BF16), vmem((2, r2, embed), F32),
        vmem((r2, embed), BF16), vmem((r2, embed), BF16), vmem(far[1:], F32),
        vmem((high, r3, embed), BF16), vmem((high, r3, embed), BF16),
        vmem((2, parts) + far, BF16), vmem((rounds, 8, LANES), F32),
    ]
    scratch += [dma((n,)) for n in (4, 2)]
    scratch += [dma((n,)) for n in (high, high, LOW, LOW, high, high, LOW, LOW)]
    scratch += [dma((n,)) for n in (high, high, high, high, LOW, LOW)]
    scratch += [dma((n,)) for n in (1, 1, parts, parts, 1, 1, high, high)]
    scratch += [dma((n,)) for n in (rounds, rounds, high, high, parts, parts, parts, parts, 1, 1)]
    space = pltpu.VMEM
    grad, loss = pl.pallas_call(
        functools.partial(kernel, high, parts),
        out_shape=(
            jax.ShapeDtypeStruct((2, parts) + far, BF16),
            jax.ShapeDtypeStruct((1, 1), F32),
        ),
        in_specs=[
            pl.BlockSpec(memory_space=space)
            for space in (pl.ANY, pl.ANY, space, space, space, pl.ANY, pl.ANY)
        ],
        out_specs=(pl.BlockSpec(memory_space=pl.ANY), pl.BlockSpec(memory_space=space)),
        scratch_shapes=scratch,
        compiler_params=pltpu.CompilerParams(
            collective_id=0, has_side_effects=True, vmem_limit_bytes=60 * 1024 * 1024
        ),
        name="two_tower",
    )(
        query_feats[0], item_feats[0], item_ids, bucket_ids, bucket_logq[None, :], query_tower, item_tower
    )
    grad = grad.reshape(2, width, embed).astype(F32)
    return grad[0], grad[1], loss.reshape(())


def solution(mesh):
    high = mesh.shape["blk"] // LOW
    return jax.shard_map(
        functools.partial(on_device, high, mesh.shape["dp"]),
        mesh=mesh,
        in_specs=(
            P("dp", "blk", None), P("dp", "blk", None), P("dp", "blk"), P("dp", "blk"), P(), P(), P(),
        ),
        out_specs=(P(), P(), P()),
        check_vma=False,
    )
```
